32 devices in a mesh: grp: 8 (over z, core), tp: 4 (over y, x).
Axes of the slice: x: 2, y: 2, z: 4, core: 2. Of those that a mesh axis runs over, the one named last changes fastest.
Arguments:
- queries: bfloat16 [8, 4, 512, 8192], P('grp', None, None, 'tp'), may hold values from -6 to 6
- keys: bfloat16 [8, 4, 512, 1024], P('grp', None, None, 'tp'), may hold values from -6 to 6
- values: bfloat16 [8, 4, 512, 1024], P('grp', None, None, 'tp'), may hold values from -6 to 6
- plan: int32 [8, 4], P('grp'), may hold values from 0 to 1, as said below
- page_table: int32 [8, 32], P('grp'), may hold values from 0 to 31, each once within a row
- refs: int32 [8], P('grp'), may hold values from 1 to 8
Outputs:
- attended: bfloat16 [8, 4, 512, 8192], P('grp', None, None, 'tp')
- page_cache: bfloat16 [8, 4, 2, 512, 1024], P('grp', None, None, None, 'tp')
- page_scales: float32 [8, 4, 2, 512], P('grp')
- layer_refs: int32 [4], replicated
The draws below stay inside these ranges and needn't reach their ends.
Inputs may be any that keep to these rules, and one draw needn't show every extreme that they name: Each row g >= 1 of plan holds exactly one 1; row 0 is not used. Each row of page_table is a permutation of the slots.
All inputs are finite; a program needn't handle non-finite values. Where the reference program divides by a largest or mean magnitude, that divisor is 1e-20 or more.
Results may differ from the reference program's by a relative error of at most 0.012.
The reference program's roundings to bfloat16 on the way count: a program that leaves them out, or rounds other values in their place, can miss the bound.
Values may be sent and summed in bfloat16 or wider, within the bound.
A program may use at most 192 MiB of HBM per device.

```python
import math
import jax
import jax.numpy as jnp
from jax import lax

ROWS = 512
LAYERS = 4
MOST = 1
KVH = 8
QPK = 8
HEAD = 128
PAGE = 16
PAGES = 32
QHEADS = 64
N_GRP = 8


def draw_keys(key, part):
    shape = (N_GRP, LAYERS, ROWS, KVH * HEAD)
    base = jnp.clip(jax.random.normal(jax.random.fold_in(key, 3), shape, jnp.float32), -6.0, 6.0)
    return base.astype(jnp.bfloat16)


def draw_queries(key, part):
    shape = (N_GRP, LAYERS, ROWS, QHEADS * HEAD)
    base = jnp.clip(jax.random.normal(jax.random.fold_in(key, 5), shape, jnp.float32), -6.0, 6.0)
    return base.astype(jnp.bfloat16)


def draw_plan(key, part):
    tiebreak = jax.random.randint(jax.random.fold_in(key, 21), (N_GRP, LAYERS), 0, 1048576) * LAYERS + jnp.arange(LAYERS)[None, :]
    ranking = jnp.argsort(jnp.argsort(tiebreak, axis=1), axis=1)
    return (ranking < MOST).astype(jnp.int32)


def with_ends(array, stream_key, least, largest):
    longest = array.shape.index(max(array.shape))
    spots = []
    for shift in (0, 1):
        where = [jax.random.randint(jax.random.fold_in(stream_key, axis), (), 0, length) for axis, length in enumerate(array.shape)]
        where[longest] = (where[longest] + shift) % array.shape[longest]
        spots.append(tuple(where))
    return array.at[spots[0]].set(least).at[spots[1]].set(largest)


def block_levels(rng, dims, shards, least, high):
    loudness = 1.0
    for position, blocks in shards:
        heights = jax.random.uniform(jax.random.fold_in(jax.random.fold_in(rng, 6), position), (blocks,), jnp.float32, least / len(shards), high / len(shards))
        loudness = loudness * jnp.repeat(jnp.exp(heights), dims[position] // blocks).reshape((-1,) + (1,) * (len(dims) - 1 - position))
    return loudness


def normal_values(key, extent, width, limit, cuts=(), held_as=jnp.bfloat16):
    values = jax.random.normal(key, extent, jnp.float32) * width
    if len(cuts) > 0:
        values = block_levels(key, extent, cuts, -0.22, 0.18) * values
    return jnp.clip(values, min=-limit, max=limit).astype(held_as)


def setup_inputs(seed: int = 0) -> dict:
    key_of = jax.random.split(jax.random.key(seed), 7)
    queries = draw_queries(jax.random.fold_in(key_of[6], 71), 0)
    keys = draw_keys(jax.random.fold_in(key_of[6], 71), 0)
    values = normal_values(key_of[2], (N_GRP, LAYERS, ROWS, KVH * HEAD), 1.0, 6.0, ((0, 8), (3, 4)))
    plan = draw_plan(jax.random.fold_in(key_of[6], 71), 0)
    page_table = jax.vmap(lambda own: jax.random.permutation(own, PAGES))(jax.random.split(key_of[4], N_GRP)).reshape((N_GRP, PAGES)).astype(jnp.int32)
    refs = with_ends(jax.random.randint(key_of[5], (N_GRP,), 1, 9), jax.random.fold_in(key_of[5], 1), 1, 8).astype(jnp.int32)
    return dict(queries=queries, keys=keys, values=values, plan=plan, page_table=page_table, refs=refs)


def rotary(tensor, offset, head_count):
    half_size = HEAD // 2
    frequency = jnp.exp(jnp.arange(half_size, dtype=jnp.float32) * (-2.0 * math.log(500000.0) / HEAD))
    places = offset + jnp.arange(tensor.shape[-2], dtype=jnp.float32)
    angles = places[:, None] * frequency[None, :]
    cosines = jnp.cos(angles)[:, None, :]
    sines = jnp.sin(angles)[:, None, :]
    shaped = tensor.astype(jnp.float32).reshape(tensor.shape[:-1] + (head_count, HEAD))
    front_half = shaped[..., :half_size]
    back_half = shaped[..., half_size:]
    turned = jnp.concatenate([front_half * cosines - back_half * sines, back_half * cosines + front_half * sines], axis=-1)
    return turned.reshape(tensor.shape).astype(jnp.bfloat16)

def quantize(tensor, scales):
    ratio = tensor.astype(jnp.float32) * 127.0 / scales.astype(jnp.float32)[..., None]
    return jnp.clip(jnp.floor(ratio + 0.5), -127.0, 127.0).astype(jnp.bfloat16)

def restore(stored, scales):
    held = lax.optimization_barrier(stored)
    return (held.astype(jnp.float32) * scales.astype(jnp.float32)[..., None] / 127.0).astype(jnp.bfloat16)

def form_pages(keys_group, values_group, offset):
    roped = rotary(keys_group, offset, KVH)
    raw_pages = jnp.stack([roped, values_group], axis=1)
    scales = jnp.maximum(lax.optimization_barrier(jnp.max(jnp.abs(raw_pages), axis=-1)), jnp.bfloat16(1.0))
    stored = quantize(raw_pages, scales)
    return (stored, scales, restore(stored, scales))

def attend_layer(queries_layer, own_pages, prompt_pages, use_prompt):
    row_count = queries_layer.shape[0]
    score_scale = 1.0 / math.sqrt(HEAD)
    split_queries = queries_layer.reshape(row_count, KVH, QPK, HEAD).transpose(1, 0, 2, 3)
    split_own = own_pages.reshape(2, row_count, KVH, HEAD).transpose(2, 0, 1, 3)
    split_prompt = prompt_pages.reshape(2, row_count, KVH, HEAD).transpose(2, 0, 1, 3)
    causal = jnp.arange(row_count)[:, None] >= jnp.arange(row_count)[None, :]

    def one_head(items):
        head_queries, head_own, head_prompt = items
        query_wide = head_queries.astype(jnp.float32)
        own_scores = jnp.einsum('iqd,jd->qij', query_wide, head_own[0].astype(jnp.float32)) * score_scale
        own_scores = jnp.where(causal[None], own_scores, -jnp.inf)
        own_top = lax.optimization_barrier(jnp.max(own_scores, axis=-1))

        def with_prompt(top):
            prompt_scores = jnp.einsum('iqd,jd->qij', query_wide, head_prompt[0].astype(jnp.float32)) * score_scale
            top_all = jnp.maximum(top, lax.optimization_barrier(jnp.max(prompt_scores, axis=-1)))
            weights = jnp.exp(prompt_scores - top_all[..., None]).astype(jnp.bfloat16)
            weights = lax.optimization_barrier(weights).astype(jnp.float32)
            totals = jnp.einsum('qij,jd->qid', weights, head_prompt[1].astype(jnp.float32))
            return (top_all, totals, lax.optimization_barrier(jnp.sum(weights, axis=-1)))

        def without_prompt(top):
            return (top, jnp.zeros((QPK, row_count, HEAD), jnp.float32), jnp.zeros((QPK, row_count), jnp.float32))
        top_all, totals, weight_sums = lax.cond(use_prompt, with_prompt, without_prompt, own_top)
        own_weights = jnp.exp(own_scores - top_all[..., None]).astype(jnp.bfloat16)
        own_weights = lax.optimization_barrier(own_weights).astype(jnp.float32)
        totals = totals + jnp.einsum('qij,jd->qid', own_weights, head_own[1].astype(jnp.float32))
        weight_sums = weight_sums + lax.optimization_barrier(jnp.sum(own_weights, axis=-1))
        return (totals / weight_sums[..., None]).transpose(1, 0, 2)
    results = lax.map(one_head, (split_queries, split_own, split_prompt))
    return results.transpose(1, 0, 2, 3).reshape(row_count, QHEADS * HEAD).astype(jnp.bfloat16)

def reference(queries, keys, values, plan, page_table, refs):
    prompt_stored, prompt_scales, prompt_cached = form_pages(keys[0], values[0], jnp.float32(0.0))

    def per_group(items):
        group_queries, group_keys, group_values, group_plan, group_table, group_id = items
        offset = jnp.where(group_id == 0, 0.0, float(ROWS)).astype(jnp.float32)
        roped_queries = rotary(group_queries, offset, QHEADS)
        own_stored, own_scales, own_cached = form_pages(group_keys, group_values, offset)
        results = []
        for layer_index in range(LAYERS):
            use_prompt = jnp.logical_and(group_id > 0, group_plan[layer_index] == 1)
            results.append(attend_layer(roped_queries[layer_index], own_cached[layer_index], prompt_cached[layer_index], use_prompt))
        attended_group = jnp.stack(results)
        holding = jnp.where(group_id == 0, 1, group_plan).astype(jnp.int32)
        slot_order = jnp.argsort(group_table).astype(jnp.int32)
        blocks = prompt_stored.reshape(LAYERS, 2, PAGES, PAGE, KVH * HEAD)
        moved = jnp.take(blocks, slot_order, axis=2).reshape(LAYERS, 2, ROWS, KVH * HEAD)
        cache_group = jnp.where(holding[:, None, None, None] == 1, moved, jnp.zeros_like(moved))
        scale_blocks = prompt_scales.astype(jnp.float32).reshape(LAYERS, 2, PAGES, PAGE)
        moved_scales = jnp.take(scale_blocks, slot_order, axis=2).reshape(LAYERS, 2, ROWS)
        scales_group = jnp.where(holding[:, None, None] == 1, moved_scales, jnp.zeros_like(moved_scales))
        return (attended_group, cache_group, scales_group)
    group_ids = jnp.arange(N_GRP).astype(jnp.int32)
    attended, page_cache, page_scales = lax.map(per_group, (queries, keys, values, plan, page_table, group_ids))
    holding_all = jnp.where(group_ids[:, None] == 0, 1, plan).astype(jnp.int32)
    layer_refs = lax.optimization_barrier(jnp.sum(refs[:, None] * holding_all, axis=0)).astype(jnp.int32)
    return (attended, page_cache, page_scales, layer_refs)
```

```python
import functools
import math

import jax
import jax.numpy as jnp
from jax import lax
from jax.experimental import pallas as pl
from jax.experimental.pallas import tpu as pltpu
from jax.sharding import PartitionSpec as P

QPK = 8
HEAD = 128
PAGE = 16
HALF = HEAD // 2
EXP2_SCALE = math.log2(math.e) / math.sqrt(HEAD)


def rotation_tables(offset, row_count):
    frequency = jnp.exp(jnp.arange(HALF, dtype=jnp.float32) * (-2.0 * math.log(500000.0) / HEAD))
    places = offset + jnp.arange(row_count, dtype=jnp.float32)
    angles = places[:, None] * frequency[None, :]
    cosines, sines = jnp.cos(angles), jnp.sin(angles)
    return (
        jnp.concatenate([cosines, cosines], axis=-1),
        jnp.concatenate([-sines, sines], axis=-1),
    )


def quantize(tensor, scales):
    ratio = tensor.astype(jnp.float32) * 127.0 / scales.astype(jnp.float32)[..., None]
    return jnp.clip(jnp.floor(ratio + 0.5), -127.0, 127.0).astype(jnp.bfloat16)


def restore(stored, scales):
    return (stored.astype(jnp.float32) * scales.astype(jnp.float32)[..., None] / 127.0).astype(
        jnp.bfloat16
    )


def rotate(tile, cosines, sines):
    wide = tile.astype(jnp.float32)
    return (wide * cosines + pltpu.roll(wide, HALF, 1) * sines).astype(jnp.bfloat16)


def row_tile(row_count):
    return 256 if row_count % 256 == 0 else row_count


def rope_body(keys_ref, cos_ref, sin_ref, out_ref):
    for head in range(keys_ref.shape[-1] // HEAD):
        lanes = slice(head * HEAD, (head + 1) * HEAD)
        out_ref[0, :, lanes] = rotate(keys_ref[0, 0, :, lanes], cos_ref[...], sin_ref[...])


def rope_keys(keys, cosines, sines):
    _, layers, rows, width = keys.shape
    return pl.pallas_call(
        rope_body,
        grid=(layers,),
        in_specs=[
            pl.BlockSpec((1, 1, rows, width), lambda l: (0, l, 0, 0)),
            pl.BlockSpec((rows, HEAD), lambda l: (0, 0)),
            pl.BlockSpec((rows, HEAD), lambda l: (0, 0)),
        ],
        out_specs=pl.BlockSpec((1, rows, width), lambda l: (l, 0, 0)),
        out_shape=jax.ShapeDtypeStruct((layers, rows, width), jnp.bfloat16),
    )(keys, cosines, sines)


def attend_rows(q_ref, own_ref, prompt_ref, cos_ref, sin_ref, out_ref):
    rows = q_ref.shape[2]
    tile = row_tile(rows)
    own_keys = own_ref[0, 0]
    ones = jnp.ones((rows, HEAD), jnp.bfloat16)
    own_values = jnp.concatenate([own_ref[0, 1], ones], axis=1)
    if prompt_ref is not None:
        prompt_keys = prompt_ref[0]
        prompt_values = jnp.concatenate([prompt_ref[1], ones], axis=1)
    causal = lax.broadcasted_iota(jnp.int32, (tile, tile), 0) >= lax.broadcasted_iota(
        jnp.int32, (tile, tile), 1
    )
    contract = (((1,), (1,)), ((), ()))
    for block in range(rows // tile):
        first = block * tile
        cosines = cos_ref[first : first + tile]
        sines = sin_ref[first : first + tile]
        for head in range(QPK):
            lanes = slice(head * HEAD, (head + 1) * HEAD)
            query = rotate(q_ref[0, 0, first : first + tile, lanes], cosines, sines)
            parts = []
            if first > 0:
                parts.append(
                    (
                        lax.dot_general(
                            query, own_keys[:first], contract, preferred_element_type=jnp.float32
                        ),
                        own_values[:first],
                    )
                )
            near = lax.dot_general(
                query,
                own_keys[first : first + tile],
                contract,
                preferred_element_type=jnp.float32,
            )
            parts.append((jnp.where(causal, near, -jnp.inf), own_values[first : first + tile]))
            if prompt_ref is not None:
                parts.append(
                    (
                        lax.dot_general(
                            query, prompt_keys, contract, preferred_element_type=jnp.float32
                        ),
                        prompt_values,
                    )
                )
            top = functools.reduce(
                jnp.maximum, [jnp.max(scores, axis=-1, keepdims=True) for scores, _ in parts]
            )
            total = None
            for scores, values in parts:
                weights = jnp.exp2((scores - top) * EXP2_SCALE).astype(jnp.bfloat16)
                term = jnp.dot(weights, values, preferred_element_type=jnp.float32)
                total = term if total is None else total + term
            out_ref[0, 0, first : first + tile, lanes] = (
                total[:, :HEAD] / total[:, HEAD:]
            ).astype(jnp.bfloat16)


def own_body(order_ref, q_ref, own_ref, cos_ref, sin_ref, out_ref):
    attend_rows(q_ref, own_ref, None, cos_ref, sin_ref, out_ref)


def prompt_body(order_ref, q_ref, own_ref, prompt_ref, cos_ref, sin_ref, held_ref, out_ref):
    reader = order_ref[order_ref.shape[0] - 1]

    @pl.when(reader == 1)
    def _():
        attend_rows(q_ref, own_ref, prompt_ref, cos_ref, sin_ref, out_ref)

    @pl.when(reader == 0)
    def _():
        attend_rows(q_ref, own_ref, None, cos_ref, sin_ref, out_ref)


def attention(order, queries, own_cached, prompt_cached, cosines, sines, held=None):
    _, layers, rows, width = queries.shape
    kv_local = own_cached.shape[-1] // HEAD
    group_width = QPK * HEAD
    steps = layers - 1 if held is None else 1
    start = 0 if held is None else layers - 1
    q_spec = pl.BlockSpec((1, 1, rows, group_width), lambda l, k, o: (0, o[start + l], 0, k))
    own_spec = pl.BlockSpec((1, 2, rows, HEAD), lambda l, k, o: (o[start + l], 0, 0, k))
    table = pl.BlockSpec((rows, HEAD), lambda l, k, o: (0, 0))
    pair_work = rows * rows * QPK * kv_local * steps
    cost = pl.CostEstimate(
        flops=6 * HEAD * pair_work,
        bytes_accessed=4 * rows * width * steps,
        transcendentals=pair_work,
    )
    if held is None:
        body, specs, operands, aliases = own_body, [q_spec, own_spec], [queries, own_cached], {}
    else:
        body = prompt_body
        specs = [q_spec, own_spec, pl.BlockSpec((2, rows, HEAD), lambda l, k, o: (0, 0, k))]
        operands = [queries, own_cached, prompt_cached]
        aliases = {6: 0}
    specs = specs + [table, table]
    operands = operands + [cosines, sines]
    if held is not None:
        specs.append(pl.BlockSpec(memory_space=pl.ANY))
        operands.append(held)
    return pl.pallas_call(
        body,
        grid_spec=pltpu.PrefetchScalarGridSpec(
            num_scalar_prefetch=1,
            grid=(steps, kv_local),
            in_specs=specs,
            out_specs=q_spec,
        ),
        out_shape=jax.ShapeDtypeStruct(queries.shape, jnp.bfloat16),
        input_output_aliases=aliases,
        cost_estimate=cost,
    )(order, *operands)


def pages_body(control_ref, own_ref, prompt_ref, out_ref):
    layer = pl.program_id(0)
    layers = pl.num_programs(0)
    sides = out_ref.shape[1]
    pages = out_ref.shape[2] // PAGE
    holds = control_ref[pages + layer]
    reader = control_ref[pages + layers]

    def place(read):
        for page in range(pages):
            slot = pl.multiple_of(control_ref[page] * PAGE, PAGE)
            for side in range(sides):
                out_ref[0, side, pl.ds(slot, PAGE), :] = read(side, page)

    @pl.when(holds == 0)
    def _():
        out_ref[...] = jnp.zeros_like(out_ref)

    @pl.when((holds == 1) & (reader == 0))
    def _():
        place(lambda side, page: own_ref[0, side, page * PAGE : (page + 1) * PAGE, :])

    @pl.when((holds == 1) & (reader == 1))
    def _():
        place(lambda side, page: prompt_ref[side, page * PAGE : (page + 1) * PAGE, :])


def place_pages(control, own_stored, prompt_stored):
    layers, sides, rows, width = own_stored.shape
    switch = control.shape[0] - 1
    return pl.pallas_call(
        pages_body,
        grid_spec=pltpu.PrefetchScalarGridSpec(
            num_scalar_prefetch=1,
            grid=(layers,),
            in_specs=[
                pl.BlockSpec(
                    (1, sides, rows, width), lambda l, c: (l * (1 - c[switch]), 0, 0, 0)
                ),
                pl.BlockSpec((sides, rows, width), lambda l, c: (0, 0, 0)),
            ],
            out_specs=pl.BlockSpec((1, sides, rows, width), lambda l, c: (l, 0, 0, 0)),
        ),
        out_shape=jax.ShapeDtypeStruct(own_stored.shape, jnp.bfloat16),
    )(control, own_stored, prompt_stored)


def parcels_body(wanted_ref, stored_ref, tail_ref, *out_refs):
    rows = stored_ref.shape[2]
    for place, out_ref in enumerate(out_refs):
        layer = wanted_ref[place + 1]
        out_ref[:, :rows, :] = stored_ref[layer]
        out_ref[:, rows:, :] = tail_ref[layer]


def pack_parcels(wanted, stored, tail):
    layers, sides, rows, width = stored.shape
    tail_rows = tail.shape[2]
    parcel = (sides, rows + tail_rows, width)
    count = wanted.shape[0] - 1
    return pl.pallas_call(
        parcels_body,
        grid_spec=pltpu.PrefetchScalarGridSpec(
            num_scalar_prefetch=1,
            grid=(1,),
            in_specs=[
                pl.BlockSpec(stored.shape, lambda i, w: (0, 0, 0, 0)),
                pl.BlockSpec(tail.shape, lambda i, w: (0, 0, 0, 0)),
            ],
            out_specs=[pl.BlockSpec(parcel, lambda i, w: (0, 0, 0))] * count,
        ),
        out_shape=[jax.ShapeDtypeStruct(parcel, jnp.bfloat16)] * count,
    )(wanted, stored, tail)


def local(groups, queries, keys, values, plan, page_table, refs):
    group_index = lax.axis_index("grp")
    layers, row_count, width = keys.shape[1:]
    page_count = row_count // PAGE
    offset = jnp.where(group_index == 0, 0.0, float(row_count)).astype(jnp.float32)
    cosines, sines = rotation_tables(offset, row_count)
    roped_keys = rope_keys(keys, cosines, sines)
    own_raw = jnp.stack([roped_keys, values[0]], axis=1)
    own_top = lax.pmax(jnp.max(jnp.abs(own_raw), axis=-1), "tp")
    own_scale = jnp.maximum(own_top, jnp.bfloat16(1.0))
    own_stored = quantize(own_raw, own_scale)
    own_cached = restore(own_stored, own_scale)

    notes = lax.all_gather(jnp.concatenate([plan[0], refs]), "grp")
    all_plans = jnp.where(jnp.arange(groups)[:, None] == 0, 1, notes[:, :layers])
    layer_refs = jnp.sum(all_plans * notes[:, layers:], axis=0).astype(jnp.int32)
    wanted = jnp.argmax(notes[:, :layers], axis=1).astype(jnp.int32)

    scale_rows = -(-row_count // (width * PAGE)) * PAGE
    scale_tail = jnp.pad(own_scale, ((0, 0), (0, 0), (0, scale_rows * width - row_count)))
    scale_tail = scale_tail.reshape(layers, 2, scale_rows, width)
    prompt_stored = jnp.zeros((2, row_count, width), jnp.bfloat16)
    prompt_tail = jnp.zeros((2, scale_rows, width), jnp.bfloat16)
    parcels = pack_parcels(wanted, own_stored, scale_tail)
    for group in range(1, groups):
        chosen = parcels[group - 1]
        came = lax.ppermute(chosen, "grp", [(0, group)])
        mine = group_index == group
        prompt_stored = jnp.where(mine, came[:, :row_count], prompt_stored)
        prompt_tail = jnp.where(mine, came[:, row_count:], prompt_tail)
    prompt_scale = prompt_tail.reshape(2, scale_rows * width)[:, :row_count]
    prompt_cached = restore(prompt_stored, prompt_scale)

    reader = (group_index > 0).astype(jnp.int32)
    favoured = jnp.argmax(plan[0]).astype(jnp.int32)
    places = jnp.arange(layers - 1, dtype=jnp.int32)
    order = jnp.concatenate(
        [places + (places >= favoured).astype(jnp.int32), favoured[None], reader[None]]
    )
    partial = attention(order, queries, own_cached, None, cosines, sines)
    attended = attention(order, queries, own_cached, prompt_cached, cosines, sines, partial)

    holding = jnp.where(group_index == 0, 1, plan[0])
    control = jnp.concatenate([page_table[0], holding, reader[None]])
    page_cache = place_pages(control, own_stored, prompt_stored)[None]

    placing = page_table[0][None, :] == jnp.arange(page_count)[:, None]
    any_scale = jnp.where(group_index == 0, own_scale, prompt_scale[None]).astype(jnp.float32)
    scale_blocks = any_scale.reshape(layers, 2, 1, page_count, PAGE)
    moved_scales = jnp.sum(jnp.where(placing[None, None, :, :, None], scale_blocks, 0.0), axis=3)
    moved_scales = moved_scales.reshape(layers, 2, row_count)
    page_scales = jnp.where(holding[:, None, None] == 1, moved_scales, 0.0)[None]
    return (attended, page_cache, page_scales, layer_refs)


def solution(mesh):
    placed = (
        P("grp", None, None, "tp"),
        P("grp", None, None, "tp"),
        P("grp", None, None, "tp"),
        P("grp", None),
        P("grp", None),
        P("grp"),
    )
    return jax.shard_map(
        functools.partial(local, mesh.shape["grp"]),
        mesh=mesh,
        in_specs=placed,
        out_specs=(
            P("grp", None, None, "tp"),
            P("grp", None, None, None, "tp"),
            P("grp", None, None, None),
            P(),
        ),
        check_vma=False,
    )
```

```python
import functools
import math

import jax
import jax.numpy as jnp
from jax import lax
from jax.experimental import pallas as pl
from jax.experimental.pallas import tpu as pltpu
from jax.sharding import PartitionSpec as P

QPK = 8
HEAD = 128
PAGE = 16
HALF = HEAD // 2
EXP2_SCALE = math.log2(math.e) / math.sqrt(HEAD)


def rotation_tables(offset, row_count):
    lane = jnp.arange(HEAD, dtype=jnp.int32)
    place_in_half = (lane % HALF).astype(jnp.float32)
    frequency = jnp.exp(place_in_half * (-2.0 * math.log(500000.0) / HEAD))
    places = offset + jnp.arange(row_count, dtype=jnp.float32)
    angles = places[:, None] * frequency[None, :]
    sign = jnp.where(lane < HALF, -1.0, 1.0)
    return jnp.cos(angles), jnp.sin(angles) * sign[None, :]


def planned_layer(control_ref, layers):
    chosen = layers - 1
    for layer in reversed(range(layers)):
        chosen = jnp.where(control_ref[layer] == 1, layer, chosen)
    return chosen


def quantize(tensor, scales):
    ratio = tensor.astype(jnp.float32) * 127.0 / scales.astype(jnp.float32)[..., None]
    return jnp.clip(jnp.floor(ratio + 0.5), -127.0, 127.0).astype(jnp.bfloat16)


def restore(stored, scales):
    return (stored.astype(jnp.float32) * scales.astype(jnp.float32)[..., None] / 127.0).astype(
        jnp.bfloat16
    )


def rotate(tile, cosines, sines):
    wide = tile.astype(jnp.float32)
    return (wide * cosines + pltpu.roll(wide, HALF, 1) * sines).astype(jnp.bfloat16)


def row_tile(row_count):
    return 256 if row_count % 256 == 0 else row_count


def rope_body(keys_ref, cos_ref, sin_ref, out_ref):
    for head in range(keys_ref.shape[-1] // HEAD):
        lanes = slice(head * HEAD, (head + 1) * HEAD)
        out_ref[0, :, lanes] = rotate(keys_ref[0, 0, :, lanes], cos_ref[...], sin_ref[...])


def rope_keys(keys, cosines, sines):
    _, layers, rows, width = keys.shape
    return pl.pallas_call(
        rope_body,
        grid=(layers,),
        in_specs=[
            pl.BlockSpec((1, 1, rows, width), lambda l: (0, l, 0, 0)),
            pl.BlockSpec((rows, HEAD), lambda l: (0, 0)),
            pl.BlockSpec((rows, HEAD), lambda l: (0, 0)),
        ],
        out_specs=pl.BlockSpec((1, rows, width), lambda l: (l, 0, 0)),
        out_shape=jax.ShapeDtypeStruct((layers, rows, width), jnp.bfloat16),
    )(keys, cosines, sines)


def attend_rows(q_ref, own_ref, prompt_ref, cos_ref, sin_ref, out_ref):
    rows = q_ref.shape[2]
    tile = row_tile(rows)
    own_keys = own_ref[0, 0]
    ones = jnp.ones((rows, HEAD), jnp.bfloat16)
    own_values = jnp.concatenate([own_ref[0, 1], ones], axis=1)
    if prompt_ref is not None:
        prompt_keys = prompt_ref[0]
        prompt_values = jnp.concatenate([prompt_ref[1], ones], axis=1)
    causal = lax.broadcasted_iota(jnp.int32, (tile, tile), 0) >= lax.broadcasted_iota(
        jnp.int32, (tile, tile), 1
    )
    contract = (((1,), (1,)), ((), ()))
    for block in range(rows // tile):
        first = block * tile
        cosines = cos_ref[first : first + tile]
        sines = sin_ref[first : first + tile]
        for head in range(QPK):
            lanes = slice(head * HEAD, (head + 1) * HEAD)
            query = rotate(q_ref[0, 0, first : first + tile, lanes], cosines, sines)
            parts = []
            if first > 0:
                parts.append(
                    (
                        lax.dot_general(
                            query, own_keys[:first], contract, preferred_element_type=jnp.float32
                        ),
                        own_values[:first],
                    )
                )
            near = lax.dot_general(
                query,
                own_keys[first : first + tile],
                contract,
                preferred_element_type=jnp.float32,
            )
            parts.append((jnp.where(causal, near, -jnp.inf), own_values[first : first + tile]))
            if prompt_ref is not None:
                parts.append(
                    (
                        lax.dot_general(
                            query, prompt_keys, contract, preferred_element_type=jnp.float32
                        ),
                        prompt_values,
                    )
                )
            top = functools.reduce(
                jnp.maximum, [jnp.max(scores, axis=-1, keepdims=True) for scores, _ in parts]
            )
            total = None
            for scores, values in parts:
                weights = jnp.exp2((scores - top) * EXP2_SCALE).astype(jnp.bfloat16)
                term = jnp.dot(weights, values, preferred_element_type=jnp.float32)
                total = term if total is None else total + term
            out_ref[0, 0, first : first + tile, lanes] = (
                total[:, :HEAD] / total[:, HEAD:]
            ).astype(jnp.bfloat16)


def own_body(order_ref, q_ref, own_ref, cos_ref, sin_ref, out_ref):
    attend_rows(q_ref, own_ref, None, cos_ref, sin_ref, out_ref)


def prompt_body(order_ref, q_ref, own_ref, prompt_ref, cos_ref, sin_ref, held_ref, out_ref):
    reader = order_ref[order_ref.shape[0] - 1]

    @pl.when(reader == 1)
    def _():
        attend_rows(q_ref, own_ref, prompt_ref, cos_ref, sin_ref, out_ref)

    @pl.when(reader == 0)
    def _():
        attend_rows(q_ref, own_ref, None, cos_ref, sin_ref, out_ref)


def attention(control, queries, own_cached, prompt_cached, cosines, sines, held=None):
    _, layers, rows, width = queries.shape
    kv_local = own_cached.shape[-1] // HEAD
    group_width = QPK * HEAD
    steps = layers - 1 if held is None else 1

    def layer_of(step, control_ref):
        planned = planned_layer(control_ref, layers)
        if held is not None:
            return planned
        return jnp.where(step >= planned, step + 1, step)

    q_spec = pl.BlockSpec((1, 1, rows, group_width), lambda l, k, o: (0, layer_of(l, o), 0, k))
    own_spec = pl.BlockSpec((1, 2, rows, HEAD), lambda l, k, o: (layer_of(l, o), 0, 0, k))
    table = pl.BlockSpec((rows, HEAD), lambda l, k, o: (0, 0))
    pair_work = rows * rows * QPK * kv_local * steps
    cost = pl.CostEstimate(
        flops=6 * HEAD * pair_work,
        bytes_accessed=4 * rows * width * steps,
        transcendentals=pair_work,
    )
    if held is None:
        body, specs, operands, aliases = own_body, [q_spec, own_spec], [queries, own_cached], {}
    else:
        body = prompt_body
        specs = [q_spec, own_spec, pl.BlockSpec((2, rows, HEAD), lambda l, k, o: (0, 0, k))]
        operands = [queries, own_cached, prompt_cached]
        aliases = {6: 0}
    specs = specs + [table, table]
    operands = operands + [cosines, sines]
    if held is not None:
        specs.append(pl.BlockSpec(memory_space=pl.ANY))
        operands.append(held)
    return pl.pallas_call(
        body,
        grid_spec=pltpu.PrefetchScalarGridSpec(
            num_scalar_prefetch=1,
            grid=(steps, kv_local),
            in_specs=specs,
            out_specs=q_spec,
        ),
        out_shape=jax.ShapeDtypeStruct(queries.shape, jnp.bfloat16),
        input_output_aliases=aliases,
        cost_estimate=cost,
    )(control, *operands)


def pages_body(control_ref, own_ref, prompt_ref, out_ref):
    layer = pl.program_id(0)
    layers = control_ref.shape[0] - 1 - out_ref.shape[2] // PAGE
    sides = out_ref.shape[1]
    pages = out_ref.shape[2] // PAGE
    reader = control_ref[control_ref.shape[0] - 1]
    holds = jnp.where(reader == 0, 1, control_ref[layer])

    def place(read):
        for page in range(pages):
            slot = pl.multiple_of(control_ref[layers + page] * PAGE, PAGE)
            for side in range(sides):
                out_ref[0, side, pl.ds(slot, PAGE), :] = read(side, page)

    @pl.when(holds == 0)
    def _():
        out_ref[...] = jnp.zeros_like(out_ref)

    @pl.when((holds == 1) & (reader == 0))
    def _():
        place(lambda side, page: own_ref[0, side, page * PAGE : (page + 1) * PAGE, :])

    @pl.when((holds == 1) & (reader == 1))
    def _():
        place(lambda side, page: prompt_ref[side, page * PAGE : (page + 1) * PAGE, :])


def place_pages(control, own_stored, prompt_stored):
    layers, sides, rows, width = own_stored.shape
    switch = control.shape[0] - 1
    return pl.pallas_call(
        pages_body,
        grid_spec=pltpu.PrefetchScalarGridSpec(
            num_scalar_prefetch=1,
            grid=(layers,),
            in_specs=[
                pl.BlockSpec(
                    (1, sides, rows, width), lambda l, c: (l * (1 - c[switch]), 0, 0, 0)
                ),
                pl.BlockSpec((sides, rows, width), lambda l, c: (0, 0, 0)),
            ],
            out_specs=pl.BlockSpec((1, sides, rows, width), lambda l, c: (l, 0, 0, 0)),
        ),
        out_shape=jax.ShapeDtypeStruct(own_stored.shape, jnp.bfloat16),
    )(control, own_stored, prompt_stored)


def parcels_body(wanted_ref, stored_ref, tail_ref, *out_refs):
    rows = stored_ref.shape[2]
    for place, out_ref in enumerate(out_refs):
        layer = wanted_ref[place + 1]
        out_ref[:, :rows, :] = stored_ref[layer]
        out_ref[:, rows:, :] = tail_ref[layer]


def pack_parcels(wanted, stored, tail):
    layers, sides, rows, width = stored.shape
    tail_rows = tail.shape[2]
    parcel = (sides, rows + tail_rows, width)
    count = wanted.shape[0] - 1
    return pl.pallas_call(
        parcels_body,
        grid_spec=pltpu.PrefetchScalarGridSpec(
            num_scalar_prefetch=1,
            grid=(1,),
            in_specs=[
                pl.BlockSpec(stored.shape, lambda i, w: (0, 0, 0, 0)),
                pl.BlockSpec(tail.shape, lambda i, w: (0, 0, 0, 0)),
            ],
            out_specs=[pl.BlockSpec(parcel, lambda i, w: (0, 0, 0))] * count,
        ),
        out_shape=[jax.ShapeDtypeStruct(parcel, jnp.bfloat16)] * count,
    )(wanted, stored, tail)


def local(groups, queries, keys, values, plan, page_table, refs):
    group_index = lax.axis_index("grp")
    layers, row_count, width = keys.shape[1:]
    page_count = row_count // PAGE
    offset = jnp.where(group_index == 0, 0.0, float(row_count)).astype(jnp.float32)
    cosines, sines = rotation_tables(offset, row_count)
    roped_keys = rope_keys(keys, cosines, sines)
    own_raw = jnp.stack([roped_keys, values[0]], axis=1)
    own_top = lax.pmax(jnp.max(jnp.abs(own_raw), axis=-1), "tp")
    own_scale = jnp.maximum(own_top, jnp.bfloat16(1.0))
    own_stored = quantize(own_raw, own_scale)
    own_cached = restore(own_stored, own_scale)

    notes = lax.all_gather(jnp.concatenate([plan[0], refs]), "grp")
    all_plans = jnp.where(jnp.arange(groups)[:, None] == 0, 1, notes[:, :layers])
    layer_refs = jnp.sum(all_plans * notes[:, layers:], axis=0).astype(jnp.int32)
    wanted = jnp.argmax(notes[:, :layers], axis=1).astype(jnp.int32)

    scale_rows = -(-row_count // (width * PAGE)) * PAGE
    scale_tail = jnp.pad(own_scale, ((0, 0), (0, 0), (0, scale_rows * width - row_count)))
    scale_tail = scale_tail.reshape(layers, 2, scale_rows, width)
    prompt_stored = jnp.zeros((2, row_count, width), jnp.bfloat16)
    prompt_tail = jnp.zeros((2, scale_rows, width), jnp.bfloat16)
    parcels = pack_parcels(wanted, own_stored, scale_tail)
    for group in range(1, groups):
        chosen = parcels[group - 1]
        came = lax.ppermute(chosen, "grp", [(0, group)])
        mine = group_index == group
        prompt_stored = jnp.where(mine, came[:, :row_count], prompt_stored)
        prompt_tail = jnp.where(mine, came[:, row_count:], prompt_tail)
    prompt_scale = prompt_tail.reshape(2, scale_rows * width)[:, :row_count]
    prompt_cached = restore(prompt_stored, prompt_scale)

    reader = (group_index > 0).astype(jnp.int32)
    control = jnp.concatenate([plan[0], page_table[0], reader[None]])
    partial = attention(control, queries, own_cached, None, cosines, sines)
    attended = attention(control, queries, own_cached, prompt_cached, cosines, sines, partial)

    holding = jnp.where(group_index == 0, 1, plan[0])
    page_cache = place_pages(control, own_stored, prompt_stored)[None]

    placing = page_table[0][None, :] == jnp.arange(page_count)[:, None]
    any_scale = jnp.where(group_index == 0, own_scale, prompt_scale[None]).astype(jnp.float32)
    scale_blocks = any_scale.reshape(layers, 2, 1, page_count, PAGE)
    moved_scales = jnp.sum(jnp.where(placing[None, None, :, :, None], scale_blocks, 0.0), axis=3)
    moved_scales = moved_scales.reshape(layers, 2, row_count)
    page_scales = jnp.where(holding[:, None, None] == 1, moved_scales, 0.0)[None]
    return (attended, page_cache, page_scales, layer_refs)


def solution(mesh):
    placed = (
        P("grp", None, None, "tp"),
        P("grp", None, None, "tp"),
        P("grp", None, None, "tp"),
        P("grp", None),
        P("grp", None),
        P("grp"),
    )
    return jax.shard_map(
        functools.partial(local, mesh.shape["grp"]),
        mesh=mesh,
        in_specs=placed,
        out_specs=(
            P("grp", None, None, "tp"),
            P("grp", None, None, None, "tp"),
            P("grp", None, None, None),
            P(),
        ),
        check_vma=False,
    )
```
